32 devices in a mesh: tok: 4 (over z), feat: 8 (over y, x, core).
Axes of the slice: x: 2, y: 2, z: 4, core: 2. Of those that a mesh axis runs over, the one named last changes fastest.
Arguments:
- tokens_in: float32 [2048, 16384], P('tok', 'feat'), may hold values from -6 to 6
- key_weight: float32 [16384, 1024], P('feat'), may hold values from -0.046875 to 0.046875
- value_weight: float32 [16384, 1024], P('feat'), may hold values from -0.046875 to 0.046875
- blocks: float32 [4, 64, 256, 256], P(None, 'feat'), may hold values from -0.25 to 1.25, as said below
- row_order: int32 [4, 128], replicated, may hold values from 0 to 127, each once within a row
- key_grad: float32 [2048, 1024], P('tok', 'feat'), may hold values from -0.3 to 0.3
- value_grad: float32 [2048, 1024], P('tok', 'feat'), may hold values from -0.3 to 0.3
- moment: float32 [4, 64, 256, 256], P(None, 'feat', 'tok'), may hold values from -1.8 to 1.8
- second_moment: float32 [4, 64, 256, 256], P(None, 'feat', 'tok'), may hold values from 0.05 to 1
Outputs:
- key_out: float32 [2048, 1024], P('tok', 'feat')
- value_out: float32 [2048, 1024], P('tok', 'feat')
- new_blocks: float32 [4, 64, 256, 256], P(None, 'feat', 'tok')
- new_moment: float32 [4, 64, 256, 256], P(None, 'feat', 'tok')
- new_second: float32 [4, 64, 256, 256], P(None, 'feat', 'tok')
The draws below stay inside these ranges and needn't reach their ends.
Inputs may be any that keep to these rules, and one draw needn't show every extreme that they name: `blocks`: every block is a dense 2 * 128 x 2 * 128 matrix. Each row of row_order is a permutation.
All inputs are finite; a program needn't handle non-finite values.
Results may differ from the reference program's by a relative error of at most 0.0001.
Values sent between devices are 32-bit elements; how exact they have to be, the bound alone decides.
No kernel may reach another device: no remote copies, remote signals or barrier semaphores. Data moves between devices by JAX's collectives and lax.ppermute only.
A program may use at most 128 MiB of HBM per device.

```python
import math
import jax
import jax.numpy as jnp
import numpy as np
from jax import lax

D = 16384
KV = 1024
HALF = 128
FACTORS = 4
TOKENS = 2048
BLOCKS = 64
N_FEAT = 8


def draw_blocks(key, part):
    noise_key, diagonal_key = jax.random.split(jax.random.fold_in(key, 17))
    shape_full = (FACTORS, BLOCKS, 2 * HALF, 2 * HALF)
    noise = jnp.clip(jax.random.normal(noise_key, shape_full, jnp.float32), -4.0, 4.0) * 0.0625
    diagonal_part = jax.random.uniform(diagonal_key, (FACTORS, BLOCKS, 2 * HALF), jnp.float32, 0.6, 1.0)
    return noise + diagonal_part[..., None] * jnp.eye(2 * HALF, dtype=jnp.float32)


def levels(own_key, shape, cuts, least, top_value):
    level = 1.0
    for position, shards_of in cuts:
        heights = jax.random.uniform(jax.random.fold_in(jax.random.fold_in(own_key, 6), position), (shards_of,), jnp.float32, least / len(cuts), top_value / len(cuts))
        level = level * jnp.repeat(jnp.exp(heights), shape[position] // shards_of).reshape((-1,) + (1,) * (len(shape) - 1 - position))
    return level


def gaussian(stream_key, shape, scale, bound, cuts=(), kind=jnp.bfloat16):
    loudness = levels(stream_key, shape, cuts, -0.22, 0.18) if cuts else 1.0
    values = jax.random.normal(stream_key, shape, jnp.float32) * scale * loudness
    return jnp.minimum(jnp.maximum(values, -bound), bound).astype(kind)


def setup_inputs(seed: int = 0) -> dict:
    splits = jax.random.split(jax.random.key(seed), 10)
    tokens_in = gaussian(splits[0], (TOKENS, D), 1.0, 6.0, ((0, 4), (1, 8)), jnp.float32)
    key_weight = gaussian(splits[1], (D, KV), D ** -0.5, 0.046875, ((0, 8),), jnp.float32)
    value_weight = gaussian(splits[2], (D, KV), D ** -0.5, 0.046875, ((0, 8),), jnp.float32)
    blocks = draw_blocks(jax.random.fold_in(splits[9], 71), 0)
    row_order = jax.vmap(lambda own: jax.random.permutation(own, HALF))(jax.random.split(splits[4], FACTORS)).reshape((FACTORS, HALF)).astype(jnp.int32)
    key_grad = gaussian(splits[5], (TOKENS, KV), 0.05, 0.3, ((0, 4), (1, 8)), jnp.float32)
    value_grad = gaussian(splits[6], (TOKENS, KV), 0.05, 0.3, ((0, 4), (1, 8)), jnp.float32)
    moment = gaussian(splits[7], (FACTORS, BLOCKS, 2 * HALF, 2 * HALF), 0.3, 1.8, ((1, 8), (2, 4)), jnp.float32)
    second_moment = jnp.clip(jnp.exp(math.log(1.0) - 2.9957323 * jax.random.uniform(splits[8], (FACTORS, BLOCKS, 2 * HALF, 2 * HALF), jnp.float32) ** levels(splits[8], (FACTORS, BLOCKS, 2 * HALF, 2 * HALF), ((1, 8), (2, 4)), -0.2, 0.2)), 0.05, 1.0)
    return {"tokens_in": tokens_in, "key_weight": key_weight, "value_weight": value_weight, "blocks": blocks, "row_order": row_order, "key_grad": key_grad, "value_grad": value_grad, "moment": moment, "second_moment": second_moment}


highest = lax.Precision.HIGHEST
beta_one = 0.9
beta_two = 0.95
learn_rate = 0.01
epsilon = 1e-08
bias_one = 1.0 - 0.9 ** 10
bias_two = 1.0 - 0.95 ** 10

def pair_tables(factor, halves_dev, feat_count):
    blocks_dev = halves_dev // 2
    bit_list = [0, 1, feat_count.bit_length() - 2]
    first_list = []
    second_list = []
    for block_index in range(blocks_dev * feat_count):
        owner_dev = block_index // blocks_dev
        slot_index = block_index % blocks_dev
        if factor == 0:
            first_half = owner_dev * halves_dev + 2 * slot_index
            second_half = first_half + 1
        else:
            stride = 1 << bit_list[factor - 1]
            if owner_dev // stride % 2 == 0:
                first_half = owner_dev * halves_dev + slot_index
                second_half = (owner_dev + stride) * halves_dev + slot_index
            else:
                first_half = (owner_dev - stride) * halves_dev + blocks_dev + slot_index
                second_half = owner_dev * halves_dev + blocks_dev + slot_index
        first_list.append(first_half)
        second_list.append(second_half)
    return (np.array(first_list, np.int32), np.array(second_list, np.int32))

def apply_factor(rotated, applied, first_index, second_index):
    token_count, width = rotated.shape
    halves = rotated.reshape(token_count, -1, HALF)
    paired = jnp.concatenate([halves[:, first_index], halves[:, second_index]], axis=2)
    turned = jnp.einsum('tbi,bij->tbj', paired, applied, precision=highest)
    result = jnp.zeros_like(halves)
    result = result.at[:, first_index].set(turned[:, :, :HALF])
    result = result.at[:, second_index].set(turned[:, :, HALF:])
    return result.reshape(token_count, width)

def reference(tokens_in, key_weight, value_weight, blocks, row_order, key_grad, value_grad, moment, second_moment):
    halves_dev = D // (HALF * N_FEAT)
    tables = [pair_tables(factor, halves_dev, N_FEAT) for factor in range(FACTORS)]

    def forward(block_values):
        rotated = tokens_in
        for factor in range(FACTORS):
            rows = jnp.concatenate([row_order[factor], row_order[factor] + HALF]).astype(jnp.int32)
            applied = jnp.take(block_values[factor], rows, axis=1)
            rotated = apply_factor(rotated, applied, tables[factor][0], tables[factor][1])
        key_part = jnp.dot(rotated, key_weight, precision=highest, preferred_element_type=jnp.float32)
        value_part = jnp.dot(rotated, value_weight, precision=highest, preferred_element_type=jnp.float32)
        return (key_part, value_part)
    outputs, pullback = jax.vjp(forward, blocks)
    key_out, value_out = outputs
    block_grad = pullback((key_grad, value_grad))[0]
    new_moment = beta_one * moment + (1.0 - beta_one) * block_grad
    new_second = beta_two * second_moment + (1.0 - beta_two) * block_grad * block_grad
    step_size = learn_rate * (new_moment / bias_one) / (jnp.sqrt(new_second / bias_two) + epsilon)
    new_blocks = blocks - step_size
    return (key_out, value_out, new_blocks, new_moment, new_second)
```

```python
import jax
import jax.numpy as jnp
from jax import lax
from jax.experimental import pallas as pl
from jax.experimental.pallas import tpu as pltpu
from jax.sharding import PartitionSpec as P


highest = lax.Precision.HIGHEST
beta_one = 0.9
beta_two = 0.95
learn_rate = 0.01
epsilon = 1e-08
bias_one = 1.0 - 0.9**10
bias_two = 1.0 - 0.95**10
f32 = jnp.float32
bf16 = jnp.bfloat16
CHUNKS = 2

NN = (((1,), (0,)), ((), ()))
NT = (((1,), (1,)), ((), ()))


def split(value):
    high = value.astype(bf16)
    low = (value - high.astype(f32)).astype(bf16)
    return high, low


def dot3(left, right, dims):
    left_high, left_low = left
    right_high, right_low = right

    (left_axis,), (right_axis,) = dims[0]
    left_all = jnp.concatenate([left_high, left_low, left_high], axis=left_axis)
    right_all = jnp.concatenate([right_low, right_high, right_high], axis=right_axis)
    return lax.dot_general(left_all, right_all, dims, preferred_element_type=f32)


def call(body, grid, in_specs, out_specs, out_shape, flops, nbytes, scratch=(), aliases=None):
    return pl.pallas_call(
        body,
        grid_spec=pltpu.PrefetchScalarGridSpec(
            num_scalar_prefetch=1,
            grid=grid,
            in_specs=in_specs,
            out_specs=out_specs,
            scratch_shapes=list(scratch),
        ),
        out_shape=out_shape,
        input_output_aliases=aliases or {},
        compiler_params=pltpu.CompilerParams(
            dimension_semantics=("arbitrary",) * len(grid), vmem_limit_bytes=32 << 20
        ),
        cost_estimate=pl.CostEstimate(
            flops=int(flops), bytes_accessed=int(nbytes), transcendentals=0
        ),
    )


def swap_send(value, axis, mask):
    return lax.ppermute(value, axis, [(i, i ^ mask) for i in range(lax.axis_size(axis))])


def prepare(info, table, blocks, first, count):
    _, blocks_dev, width, _ = blocks.shape
    half = width // 2

    def body(info_ref, table_ref, block_ref, high_ref, low_ref):
        factor = first + pl.program_id(0)
        side = info_ref[factor]
        own = pl.multiple_of(side * half, half)
        other = pl.multiple_of((1 - side) * half, half)
        perm = table_ref[0]
        for c in range(2):
            for row, row_at in ((0, own), (1, other)):
                for col, col_at in ((0, own), (1, other)):
                    piece = split(block_ref[0, c, pl.ds(row_at, half), pl.ds(col_at, half)])
                    for value, out_ref in zip(piece, (high_ref, low_ref)):
                        turned = jnp.dot(perm, value, preferred_element_type=f32)
                        out_ref[0, c, row * half : (row + 1) * half, col * half : (col + 1) * half] = (
                            turned.astype(bf16)
                        )

    spec = pl.BlockSpec((1, 2, width, width), lambda m, c, s: (m, c, 0, 0))
    shape = jax.ShapeDtypeStruct((count, blocks_dev, width, width), bf16)
    return call(
        body,
        (count, blocks_dev // 2),
        [
            pl.BlockSpec((1, half, half), lambda m, c, s: (first + m, 0, 0)),
            pl.BlockSpec((1, 2, width, width), lambda m, c, s: (first + m, c, 0, 0)),
        ],
        [spec, spec],
        [shape, shape],
        4 * count * blocks_dev * width * width * half,
        count * blocks_dev * width * width * 8,
    )(info, table, blocks)


def first_factor(info, tokens, high, low, chunk, steps):
    rows = tokens.shape[0]
    width = high.shape[-1]
    half_blocks = high.shape[1] // 2
    start = chunk * steps

    def body(info_ref, a_ref, b_ref, ah_ref, al_ref, bh_ref, bl_ref, keep_ref, send_ref):
        keep_ref[...] = dot3(split(a_ref[...]), (ah_ref[0, 0], al_ref[0, 0]), NN)
        send_ref[...] = dot3(split(b_ref[...]), (bh_ref[0, 0], bl_ref[0, 0]), NN)

    def token(flip):
        return pl.BlockSpec(
            (rows, width), lambda j, s: (0, (flip + s[1] - 2 * flip * s[1]) * half_blocks + start + j)
        )

    def block(flip):
        return pl.BlockSpec(
            (1, 1, width, width),
            lambda j, s: (0, (flip + s[1] - 2 * flip * s[1]) * half_blocks + start + j, 0, 0),
        )

    out = pl.BlockSpec((rows, width), lambda j, s: (0, j))
    shape = jax.ShapeDtypeStruct((rows, steps * width), f32)
    return call(
        body,
        (steps,),
        [token(0), token(1), block(0), block(0), block(1), block(1)],
        [out, out],
        [shape, shape],
        12 * rows * width * width * steps,
        4 * rows * width * steps * 4,
    )(info, tokens, tokens, high, low, high, low)


def pick(info_ref, refs, flag, cols=slice(None)):
    if flag is None:
        return refs[0][:, cols]
    return jnp.where(info_ref[flag] == 1, refs[0][:, cols], refs[1][:, cols])


def stage(info, kept, other, high, low, index, chunk, transposed):
    own, flag = kept
    count = len(own)
    rows, total = other.shape
    width = high.shape[-1]
    half = width // 2
    steps = total // width
    dims = NT if transposed else NN

    def body(info_ref, *refs):
        own_refs = refs[:count]
        other_ref, high_ref, low_ref, keep_ref, send_ref = refs[count:]
        for k in range(2):
            cols = slice(k * half, (k + 1) * half)
            mine = pick(info_ref, own_refs, flag, cols)
            pair = jnp.concatenate([mine, other_ref[:, cols]], axis=1)
            turned = dot3(split(pair), (high_ref[0, k], low_ref[0, k]), dims)
            keep_ref[:, cols] = turned[:, :half]
            send_ref[:, cols] = turned[:, half:]

    token = pl.BlockSpec((rows, width), lambda j, s: (0, j))
    block = pl.BlockSpec((1, 2, width, width), lambda j, s: (index, chunk * steps + j, 0, 0))
    shape = jax.ShapeDtypeStruct((rows, total), f32)
    return call(
        body,
        (steps,),
        [token] * (count + 1) + [block, block],
        [token, token],
        [shape, shape],
        12 * rows * width * width * steps,
        4 * rows * total * 4,
    )(info, *own, other, high, low)


def upstream_half(info, pieces, key_weight, value_weight, flip, chunks):
    rows, piece_width = pieces[0].shape
    columns = piece_width // 2
    features, full = key_weight.shape
    tile = 256
    half_steps = features // 2 // tile
    steps = half_steps // chunks
    count = len(pieces)

    def body(info_ref, *refs):
        piece_refs = refs[:count]
        key_ref, value_ref = refs[count : count + 2]
        out_refs = refs[count + 2 : count + 2 + chunks]
        high_ref, low_ref = refs[-2:]

        @pl.when(pl.program_id(0) == 0)
        def _():
            for p in range(count):
                high_ref[p], low_ref[p] = split(piece_refs[p][...])

        total = None
        for p in range(count):
            at = pl.multiple_of((info_ref[4] ^ p) * columns, columns)
            weight = jnp.concatenate(
                [key_ref[:, pl.ds(at, columns)], value_ref[:, pl.ds(at, columns)]], axis=1
            )
            term = dot3((high_ref[p], low_ref[p]), split(weight), NT)
            total = term if total is None else total + term
        for n in range(chunks):

            @pl.when(pl.program_id(0) // steps == n)
            def _():
                out_refs[n][...] = total

    weight = pl.BlockSpec(
        (tile, full), lambda j, s: ((flip + s[3] - 2 * flip * s[3]) * half_steps + j, 0)
    )
    return call(
        body,
        (half_steps,),
        [pl.BlockSpec((rows, piece_width), lambda j, s: (0, 0))] * count + [weight, weight],
        [
            pl.BlockSpec((rows, tile), lambda j, s, n=n: (0, jnp.clip(j - n * steps, 0, steps - 1)))
            for n in range(chunks)
        ],
        [jax.ShapeDtypeStruct((rows, steps * tile), f32)] * chunks,
        12 * rows * half_steps * tile * full * 2,
        half_steps * tile * full * 8,
        scratch=[pltpu.VMEM((count, rows, piece_width), bf16)] * 2,
    )(info, *pieces, key_weight, value_weight)


def project(info, lefts, key_weight, value_weight, core, previous, chunks):
    rows, depth = lefts[0][0].shape
    _, full = key_weight.shape
    feat_count = lax.axis_size("feat")
    columns = full // feat_count
    steps = feat_count // 2
    count = len(lefts)

    def body(info_ref, *refs):
        left_refs = refs[:count]
        weight_refs = refs[count : 3 * count]
        prev_ref = refs[3 * count] if previous is not None else None
        out_ref, high_ref, low_ref = refs[-3:]

        @pl.when(pl.program_id(0) == 0)
        def _():
            for i in range(count):
                high_ref[i], low_ref[i] = split(left_refs[i][...])

        total = prev_ref[0] if previous is not None else None
        for i in range(count):
            weight = jnp.concatenate([weight_refs[2 * i][...], weight_refs[2 * i + 1][...]], axis=1)
            term = dot3((high_ref[i], low_ref[i]), split(weight), NN)
            total = term if total is None else total + term
        out_ref[0] = total

    def weight(flip, chunk):
        return pl.BlockSpec(
            (depth, columns),
            lambda g, s: ((flip + s[3] - 2 * flip * s[3]) * chunks + chunk, s[4] ^ (2 * g + core)),
        )

    out = pl.BlockSpec((1, rows, 2 * columns), lambda g, s: (g, 0, 0))
    left = pl.BlockSpec((rows, depth), lambda g, s: (0, 0))
    weight_specs = []
    weights = []
    for _, flip, chunk in lefts:
        weight_specs += [weight(flip, chunk)] * 2
        weights += [key_weight, value_weight]
    return call(
        body,
        (steps,),
        [left] * count + weight_specs + ([out] if previous is not None else []),
        out,
        jax.ShapeDtypeStruct((steps, rows, 2 * columns), f32),
        6 * rows * depth * count * full * 2,
        depth * count * full * 4 + rows * full * 4,
        scratch=[pltpu.VMEM((count, rows, depth), bf16)] * 2,
    )(info, *[x for x, _, _ in lefts], *weights, *([previous] if previous is not None else []))


def block_gradient(info, table_back, factor, chunk, steps, left_pair, right_pair, blocks_dev, width, halving):
    half = width // 2
    half_blocks = blocks_dev // 2
    tok_count = lax.axis_size("tok")
    share = width // tok_count

    def body(info_ref, table_ref, *refs):
        ins = refs[: len(operands)]
        outs = refs[len(ins) : -1]
        acc_ref = refs[-1]
        side = info_ref[factor] if factor else None
        tok = info_ref[5]
        perm = table_ref[0]

        def finish(h, grad):
            turned = []
            for r in range(2):
                parts = split(grad[r * half : (r + 1) * half])
                turned.append(
                    jnp.dot(perm, parts[0], preferred_element_type=f32)
                    + jnp.dot(perm, parts[1], preferred_element_type=f32)
                )
            if factor:
                own = pl.multiple_of(side * half, half)
                other = pl.multiple_of((1 - side) * half, half)
                for r, row_at in ((0, own), (1, other)):
                    acc_ref[pl.ds(row_at, half), pl.ds(own, half)] = turned[r][:, :half]
                    acc_ref[pl.ds(row_at, half), pl.ds(other, half)] = turned[r][:, half:]
            else:
                acc_ref[:half] = turned[0]
                acc_ref[half:] = turned[1]
            if not halving:
                outs[0][h, 0] = acc_ref[...]
                return

            def rows_of(flip):
                return acc_ref[pl.ds(pl.multiple_of((tok ^ flip) * share, share), share), :]

            outs[0][0, h, 0] = rows_of(1)
            outs[0][1, h, 0] = rows_of(3)
            outs[1][h, 0] = rows_of(2)
            outs[2][h, 0] = rows_of(0)

        at = 0
        for k in range(2):
            if factor:
                both = []
                for (own, flag), _ in (left_pair, right_pair):
                    mine = pick(info_ref, ins[at : at + len(own)], flag)
                    both.append(jnp.concatenate([mine, ins[at + len(own)][...]], axis=1))
                    at += len(own) + 1
                left, right = both
            else:
                left = ins[at][...]
                right = ins[at + 1][...]
                at += 2
            total = dot3(split(left.T), split(right), NN)
            if factor:
                finish(k, total)
            else:
                finish(k + info_ref[1] - 2 * k * info_ref[1], total)

    operands = []
    specs = []
    for k in range(2):
        if factor:
            rows = left_pair[1].shape[0]
            for array in (*left_pair[0][0], left_pair[1], *right_pair[0][0], right_pair[1]):
                operands.append(array)
                specs.append(pl.BlockSpec((rows, half), lambda j, s, k=k: (0, k * steps + j)))
        else:
            rows = left_pair.shape[0]
            operands.append(left_pair)
            specs.append(
                pl.BlockSpec(
                    (rows, width),
                    lambda j, s, k=k: (
                        0,
                        (k + s[1] - 2 * k * s[1]) * half_blocks + chunk * steps + j,
                    ),
                )
            )
            operands.append(right_pair[k])
            specs.append(pl.BlockSpec((rows, width), lambda j, s: (0, j)))
    if halving:
        one = pl.BlockSpec((2, 1, share, width), lambda j, s: (0, j, 0, 0))
        two = pl.BlockSpec((2, 2, 1, share, width), lambda j, s: (0, 0, j, 0, 0))
        one_shape = jax.ShapeDtypeStruct((2, steps, share, width), f32)
        two_shape = jax.ShapeDtypeStruct((2, 2, steps, share, width), f32)
        outs, shapes = [two, one, one], [two_shape, one_shape, one_shape]
    else:
        outs = [pl.BlockSpec((2, 1, width, width), lambda j, s: (0, j, 0, 0))]
        shapes = [jax.ShapeDtypeStruct((2, steps, width, width), f32)]
    return call(
        body,
        (steps,),
        [pl.BlockSpec((1, half, half), lambda j, s: (factor, 0, 0))] + specs,
        outs,
        shapes,
        12 * rows * width * width * steps,
        4 * rows * width * steps * 4,
        scratch=[pltpu.VMEM((width, width), f32)],
    )(info, table_back, *operands)


def adam(info, factor, chunk, chunks, parts, blocks, moment, second, carried):
    count, blocks_dev, share, width = moment.shape
    steps = blocks_dev // 2 // chunks
    middle = (chunks, 2, steps) if factor else (2, chunks, steps)

    def view(array):
        return array.reshape(count, *middle, array.shape[-2], width)

    halving = len(parts) > 1

    def body(info_ref, *refs):
        part_refs = refs[: len(parts)]
        block_ref, moment_ref, second_ref = refs[len(parts) : len(parts) + 3]
        new_block_ref, new_moment_ref, new_second_ref = refs[-3:]
        for h in range(2):
            at = (0, 0, h, 0) if factor else (0, h, 0, 0)
            grad = part_refs[0][h, 0]
            if halving:
                grad = grad + part_refs[1][0, h, 0] + part_refs[2][h, 0]
            new_moment = beta_one * moment_ref[at] + (1.0 - beta_one) * grad
            new_second = beta_two * second_ref[at] + (1.0 - beta_two) * grad * grad
            step_size = learn_rate * (new_moment / bias_one)
            step_size = step_size / (jnp.sqrt(new_second / bias_two) + epsilon)
            new_block_ref[at] = block_ref[at] - step_size
            new_moment_ref[at] = new_moment
            new_second_ref[at] = new_second

    one = pl.BlockSpec((2, 1, share, width), lambda j, s: (0, j, 0, 0))
    part_specs = [one]
    if halving:
        part_specs += [
            pl.BlockSpec((1, 2, 1, share, width), lambda j, s: (0, 0, j, 0, 0)),
            one,
        ]
    if factor:
        state = pl.BlockSpec((1, 1, 2, 1, share, width), lambda j, s: (factor, chunk, 0, j, 0, 0))
        current = pl.BlockSpec(
            (1, 1, 2, 1, share, width), lambda j, s: (factor, chunk, 0, j, s[5], 0)
        )
    else:
        state = pl.BlockSpec((1, 2, 1, 1, share, width), lambda j, s: (0, 0, chunk, j, 0, 0))
        current = pl.BlockSpec((1, 2, 1, 1, share, width), lambda j, s: (0, 0, chunk, j, s[5], 0))
    shape = jax.ShapeDtypeStruct((count, *middle, share, width), f32)
    aliases = {}
    extra = ()
    extra_specs = []
    if carried is not None:
        extra = tuple(view(array) for array in carried)
        extra_specs = [pl.BlockSpec(memory_space=pl.ANY)] * 3
        aliases = {1 + len(parts) + 3 + i: i for i in range(3)}
    outs = call(
        body,
        (steps,),
        part_specs + [current, state, state] + extra_specs,
        [state] * 3,
        [shape] * 3,
        2 * steps * share * width * 20,
        2 * steps * share * width * 4 * 8,
        aliases=aliases,
    )(info, *parts, view(blocks), view(moment), view(second), *extra)
    return [array.reshape(moment.shape) for array in outs]


def route(info, own, other, first):
    flag = 5 + first
    return ((own, other), flag), jnp.where(info[flag] == 1, other, own)


def step(
    tokens_in,
    key_weight,
    value_weight,
    blocks,
    row_order,
    key_grad,
    value_grad,
    moment,
    second_moment,
):
    feat_count = lax.axis_size("feat")
    tok_count = lax.axis_size("tok")
    feat_index = lax.axis_index("feat")
    tok_index = lax.axis_index("tok")
    factor_count, blocks_dev, width, _ = blocks.shape
    half = width // 2
    columns = key_grad.shape[1]
    bits = [None, 0, 1, feat_count.bit_length() - 2]
    sides = [None] + [feat_index >> bits[m] & 1 for m in range(1, factor_count)]
    same = [(sides[m] == sides[m + 1]).astype(jnp.int32) for m in range(1, factor_count - 1)]
    info = jnp.stack(
        [jnp.zeros((), jnp.int32)] + sides[1:] + [feat_index, tok_index] + same
    ).astype(jnp.int32)
    lanes = jnp.arange(half, dtype=jnp.int32)
    table = (row_order[:, :, None] == lanes[None, None, :]).astype(bf16)
    table_back = (row_order[:, None, :] == lanes[None, :, None]).astype(bf16)
    chunks = CHUNKS
    steps = blocks_dev // 2 // chunks
    direct = columns % 128 == 0
    halving = tok_count == 4

    both_grad = jnp.concatenate([key_grad, value_grad], axis=1)
    if direct:
        pieces = [both_grad] + [None] * (feat_count - 1)
        for p in range(2, feat_count, 2):
            pieces[p] = swap_send(both_grad, "feat", p)
        for p in range(0, feat_count, 2):
            pieces[p + 1] = swap_send(pieces[p], "feat", 1)
    else:
        key_full = lax.all_gather(key_grad, "feat", axis=1, tiled=True)
        value_full = lax.all_gather(value_grad, "feat", axis=1, tiled=True)
        full_up = jnp.einsum("tk,dk->td", key_full, key_weight, precision=highest)
        full_up = full_up + jnp.einsum("tk,dk->td", value_full, value_weight, precision=highest)

    high_zero, low_zero = prepare(info, table, blocks, 0, 1)
    high, low = prepare(info, table, blocks, 1, factor_count - 1)

    paired = [[None] * factor_count for _ in range(chunks)]
    upstream = [[None] * factor_count for _ in range(chunks)]
    last = factor_count - 1
    for n in range(chunks):
        kept, sent = first_factor(info, tokens_in, high_zero, low_zero, n, steps)
        kept = ((kept,), None)
        for m in range(1, factor_count):
            other = swap_send(sent, "feat", 1 << bits[m])
            paired[n][m] = (kept, other)
            own, back = stage(info, kept, other, high, low, m - 1, n, False)
            other = swap_send(back, "feat", 1 << bits[m])
            if m < last:
                kept, sent = route(info, own, other, m)
            else:
                paired[n][0] = (own, other)

    if direct:
        sents = upstream_half(info, pieces, key_weight, value_weight, 1, chunks)
        keeps = upstream_half(info, pieces, key_weight, value_weight, 0, chunks)
    for n in range(chunks):
        if direct:
            sent, kept = sents[n], keeps[n]
        else:
            size = full_up.shape[1] // 2 // chunks
            low_half = full_up[:, n * size : (n + 1) * size]
            high_half = full_up[:, (chunks + n) * size : (chunks + n + 1) * size]
            kept = jnp.where(sides[last] == 1, high_half, low_half)
            sent = jnp.where(sides[last] == 1, low_half, high_half)
        kept = ((kept,), None)
        for m in range(last, 0, -1):
            other = swap_send(sent, "feat", 1 << bits[m])
            upstream[n][m] = (kept, other)
            own, back = stage(info, kept, other, high, low, m - 1, n, True)
            other = swap_send(back, "feat", 1 << bits[m])
            if m > 1:
                kept, sent = route(info, own, other, m - 1)
            else:
                upstream[n][0] = (own, other)

    if direct:
        ready = [(paired[n][0][0], 0, n) for n in range(chunks)]
        ready += [(paired[n][0][1], 1, n) for n in range(chunks - 1)]
        final = [(paired[chunks - 1][0][1], 1, chunks - 1)]
        odd = project(info, ready, key_weight, value_weight, 1, None, chunks)
        even = project(info, ready, key_weight, value_weight, 0, None, chunks)
        odd = project(info, final, key_weight, value_weight, 1, odd, chunks)
        got = swap_send(odd, "feat", 1)
        even = project(info, final, key_weight, value_weight, 0, even, chunks)
        parts = [even[g] + got[g] for g in range(feat_count // 2)]
        total = parts[0]
        for g in range(1, feat_count // 2):
            total = total + swap_send(parts[g], "feat", 2 * g)
        key_out, value_out = total[:, :columns], total[:, columns:]
    else:
        upper_side = sides[last] == 1
        owns = jnp.concatenate([paired[n][0][0] for n in range(chunks)], 1)
        others = jnp.concatenate([paired[n][0][1] for n in range(chunks)], 1)
        rotated = jnp.where(
            upper_side,
            jnp.concatenate([others, owns], 1),
            jnp.concatenate([owns, others], 1),
        )
        key_part = jnp.dot(rotated, key_weight, precision=highest, preferred_element_type=f32)
        value_part = jnp.dot(rotated, value_weight, precision=highest, preferred_element_type=f32)
        key_out = lax.psum_scatter(key_part, "feat", scatter_dimension=1, tiled=True)
        value_out = lax.psum_scatter(value_part, "feat", scatter_dimension=1, tiled=True)

    carried = None
    order = [(m, n) for pair in ((3, 2), (1, 0)) for n in range(chunks) for m in pair]
    for m, n in order:
        left = paired[n][m] if m else tokens_in
        grads = block_gradient(
            info, table_back, m, n, steps, left, upstream[n][m], blocks_dev, width, halving
        )
        if halving:
            near, hold, mine = grads
            first_in = swap_send(near, "tok", 1)
            hold = hold + first_in[1]
            second_in = swap_send(hold, "tok", 2)
            parts = [mine, first_in, second_in]
        else:
            parts = [lax.psum_scatter(grads[0], "tok", scatter_dimension=2, tiled=True)]
        carried = adam(info, m, n, chunks, parts, blocks, moment, second_moment, carried)
    new_blocks, new_moment, new_second = (a.reshape(moment.shape) for a in carried)
    return (key_out, value_out, new_blocks, new_moment, new_second)


def solution(mesh):
    placed = (
        P("tok", "feat"),
        P("feat", None),
        P("feat", None),
        P(None, "feat", None, None),
        P(),
        P("tok", "feat"),
        P("tok", "feat"),
        P(None, "feat", "tok", None),
        P(None, "feat", "tok", None),
    )
    return jax.shard_map(
        step,
        mesh=mesh,
        in_specs=placed,
        out_specs=(
            P("tok", "feat"),
            P("tok", "feat"),
            P(None, "feat", "tok", None),
            P(None, "feat", "tok", None),
            P(None, "feat", "tok", None),
        ),
        check_vma=False,
    )
```
